32 devices in a mesh: grp: 2 (over x), leaf: 16 (over z, y, core).
Axes of the slice: x: 2, y: 2, z: 4, core: 2. Of those that a mesh axis runs over, the one named last changes fastest.
Arguments:
- snapshots: float32 [131072, 256], P(('grp', 'leaf')), may hold values from -150 to 150
- sketch: float32 [256, 64], replicated, may hold values from -6 to 6
Outputs:
- recon: bfloat16 [131072, 256], P(('grp', 'leaf'))
The draws below stay inside these ranges and needn't reach their ends.
All inputs are finite; a program needn't handle non-finite values.
Results may differ from the reference program's by a relative error of at most 0.001.
Values sent between devices are 32-bit elements; how exact they have to be, the bound alone decides.
A program may use at most 64 MiB of HBM per device.

```python
import math
import jax
import jax.numpy as jnp
from jax import lax

COLS = 256
MODES = 64
ITERS = 1
ROW_DEV = 4096
ROWS = 131072
N_GRP = 2
N_LEAF = 16


def draw_snapshots(key, part):
    keys = jax.random.split(jax.random.fold_in(key, 7), 6)
    slab_count = ROWS // ROW_DEV
    position = jnp.arange(ROWS, dtype=jnp.float32) / ROWS
    row_scale = jnp.exp(position * math.log(3.0))[:, None] * jnp.exp(jax.random.uniform(keys[0], (ROWS, 1), jnp.float32, 0.0, math.log(2.0)))
    mode_index = jnp.arange(COLS, dtype=jnp.float32)
    basis_key = keys[5]
    decay = math.log(0.3) / MODES
    drop = 6.0
    loadings = jnp.clip(jax.random.normal(keys[2], (ROWS, COLS), jnp.float32), -6.0, 6.0)
    noise_level = 0.04
    col_scale = jnp.exp(jax.random.uniform(keys[1], (1, COLS), jnp.float32, 0.0, math.log(10.0)))
    orthogonal, upper = jnp.linalg.qr(jax.random.normal(basis_key, (COLS, COLS), jnp.float32))
    spectrum = jnp.exp(decay * mode_index) * jnp.where(mode_index < MODES, 1.0, 1.0 / drop)
    jitter = jnp.exp(jax.random.uniform(keys[3], (slab_count, 1, COLS), jnp.float32, -0.5 * math.log(2.0), 0.5 * math.log(2.0)))
    weighted = (loadings.reshape(slab_count, ROW_DEV, COLS) * spectrum[None, None, :] * jitter).reshape(ROWS, COLS)
    field = jnp.dot(weighted, orthogonal.T, precision=jax.lax.Precision.HIGHEST)
    noise = jnp.clip(jax.random.normal(keys[4], (ROWS, COLS), jnp.float32), -6.0, 6.0)
    values = 2.0 * (field + noise_level * noise) * col_scale * row_scale
    return jnp.clip(values, -150.0, 150.0).astype(jnp.float32)


def scatter_about(stream_key, shape, spread, bound, kind=jnp.bfloat16):
    return jnp.clip(spread * jax.random.normal(stream_key, shape, jnp.float32), -bound, bound).astype(kind)


def setup_inputs(seed: int = 0) -> dict:
    streams_of = jax.random.split(jax.random.key(seed), 3)
    snapshots = draw_snapshots(jax.random.fold_in(streams_of[2], 71), 0)
    sketch = scatter_about(streams_of[1], (COLS, MODES), 1.0, 6.0, jnp.float32)
    return {"snapshots": snapshots, "sketch": sketch}


highest_precision = lax.Precision.HIGHEST

def orthonormal(candidate):
    for repeat_index in range(2):
        correlation = jnp.dot(candidate.T, candidate, precision=highest_precision)
        lower_factor = jnp.linalg.cholesky(correlation)
        candidate = jax.scipy.linalg.solve_triangular(lower_factor, candidate.T, lower=True).T
    return candidate

def subspace(gram_sum, sketch):
    mode_basis = orthonormal(jnp.dot(gram_sum, sketch, precision=highest_precision))
    for repeat_index in range(ITERS - 1):
        mode_basis = orthonormal(jnp.dot(gram_sum, mode_basis, precision=highest_precision))
    return mode_basis

def factor(gram_sum, sketch):
    mode_basis = subspace(gram_sum, sketch)
    reduced = jnp.dot(mode_basis.T, jnp.dot(gram_sum, mode_basis, precision=highest_precision), precision=highest_precision)
    reduced = 0.5 * (reduced + reduced.T)
    lower_factor = jnp.linalg.cholesky(reduced)
    return jnp.dot(lower_factor.T, mode_basis.T, precision=highest_precision)

def reference(snapshots, sketch):
    slabs = snapshots.reshape(N_GRP * N_LEAF, ROW_DEV, COLS)

    def slab_factor(slab):
        return factor(jnp.dot(slab.T.astype(jnp.float32), slab.astype(jnp.float32), precision=highest_precision, preferred_element_type=jnp.float32), sketch)
    first_factor = lax.map(slab_factor, slabs).reshape(N_GRP, N_LEAF, MODES, COLS)
    group_gram = jnp.einsum('glmc,glmd->lcd', first_factor, first_factor, precision=highest_precision)
    second_factor = jax.vmap(lambda gram_sum: factor(gram_sum, sketch))(group_gram)
    total_gram = jnp.einsum('lmc,lmd->cd', second_factor, second_factor, precision=highest_precision)
    mode_basis = subspace(total_gram, sketch)
    projector = jnp.dot(mode_basis, mode_basis.T, precision=highest_precision)

    def project(slab):
        return jnp.dot(slab, projector, precision=highest_precision).astype(jnp.bfloat16)
    recon = lax.map(project, slabs)
    return recon.reshape(ROWS, COLS)
```

```python
import functools

import jax
import jax.numpy as jnp
from jax import lax
from jax.experimental import pallas as pl
from jax.experimental.pallas import tpu as pltpu
from jax.sharding import PartitionSpec as P

MESH = pl.DeviceIdType.MESH
VMEM = pl.BlockSpec(memory_space=pltpu.VMEM)
LANES = 128
CHUNK = 512


def dot(a, b, ca=1, cb=0):
    return lax.dot_general(
        a, b, (((ca,), (cb,)), ((), ())),
        precision=lax.Precision.HIGHEST, preferred_element_type=jnp.float32,
    )


def fast(a, b, ca=1, cb=0):
    return lax.dot_general(a, b, (((ca,), (cb,)), ((), ())), preferred_element_type=jnp.float32)


def split(x):
    hi = x.astype(jnp.bfloat16)
    return hi, (x - hi.astype(jnp.float32)).astype(jnp.bfloat16)


def identity(n):
    return (lax.broadcasted_iota(jnp.int32, (n, n), 0) == lax.broadcasted_iota(jnp.int32, (n, n), 1)).astype(jnp.float32)


def inverse_factor(c, rows_ref):
    m = c.shape[0]
    full = jnp.concatenate([c, identity(m)], axis=1)
    width = 2 * m
    blocks = [full[8 * k : 8 * k + 8] for k in range(m // 8)]
    for j in range(0, m, 2):
        k, s = j // 8, j % 8
        lead = blocks[k]
        cols = [
            (
                jnp.broadcast_to(blocks[i][:, j : j + 1], (8, width)),
                jnp.broadcast_to(blocks[i][:, j + 1 : j + 2], (8, width)),
            )
            for i in range(k, m // 8)
        ]
        r0, r1 = lead[s : s + 1], lead[s + 1 : s + 2]
        a, b, d = cols[0][0][s : s + 1], cols[0][0][s + 1 : s + 2], cols[0][1][s + 1 : s + 2]
        det = a * d - b * b
        inv = 1.0 / det
        t0 = (d * r0 - b * r1) * inv
        t1 = (a * r1 - b * r0) * inv
        for i in range(k, m // 8):
            c0, c1 = cols[i - k]
            blocks[i] = blocks[i] - c0 * t0 - c1 * t1
        ia = lax.rsqrt(a)
        rows_ref[j : j + 1, :] = r0 * ia
        rows_ref[j + 1 : j + 2, :] = (a * r1 - b * r0) * (ia * lax.rsqrt(det))
    return rows_ref[:, m:]


def orthonormal(yt, rows_ref):
    m = yt.shape[0]
    qt = dot(inverse_factor(dot(yt, yt, 1, 1), rows_ref), yt)
    err = identity(m) - dot(qt, qt, 1, 1)
    fix = 0.5 * err + 0.375 * dot(err, err)
    return qt + dot(fix, qt)


def first_kernel(x_hbm, st_ref, qt_ref, h_ref, xbuf, acc, acc2, rows_ref, sems):
    chunks = x_hbm.shape[0] // CHUNK
    cols = x_hbm.shape[1]

    def copy(i):
        at = pl.ds(pl.multiple_of(i * CHUNK, CHUNK), CHUNK)
        return pltpu.make_async_copy(x_hbm.at[at], xbuf.at[at], sems.at[i])

    for i in range(chunks):
        copy(i).start()
    acc[...] = jnp.zeros_like(acc)
    acc2[...] = jnp.zeros_like(acc2)

    def step(i, carry):
        copy(i).wait()
        hi, mid = split(xbuf[pl.ds(pl.multiple_of(i * CHUNK, CHUNK), CHUNK), :])
        acc[...] += fast(hi, jnp.concatenate([hi, mid], axis=1), 0, 0)
        acc2[...] += fast(mid, mid, 0, 0)
        return carry

    lax.fori_loop(0, chunks, step, 0)
    cross = acc[:, cols:]
    acc2[...] = acc[:, :cols] + (cross + cross.T + acc2[...])
    gram = acc2[...]
    qt = orthonormal(dot(st_ref[...], gram), rows_ref)
    qt_ref[...] = qt
    h_ref[...] = dot(dot(qt, gram), qt, 1, 1)


def entry_barrier(axis_counts):
    barrier = pltpu.get_barrier_semaphore()
    total = 0
    for axis, n in axis_counts:
        me = lax.axis_index(axis)
        for d in range(1, n):
            pl.semaphore_signal(barrier, inc=1, device_id={axis: lax.rem(me + d, n)}, device_id_type=MESH)
        total += n - 1
    pl.semaphore_wait(barrier, total)


def group_kernel(n, qt_ref, h_ref, qs_ref, hs_ref, qland, hland, qsend, qrecv, hsend, hrecv):
    entry_barrier([("grp", n)])
    me = lax.axis_index("grp")
    copies = []
    for d in range(1, n):
        peer = {"grp": lax.rem(me + d, n)}
        for src, land, ss, rs in ((qt_ref, qland, qsend, qrecv), (h_ref, hland, hsend, hrecv)):
            copies.append(
                pltpu.make_async_remote_copy(
                    src_ref=src, dst_ref=land.at[d - 1], send_sem=ss.at[d - 1], recv_sem=rs.at[d - 1],
                    device_id=peer, device_id_type=MESH,
                )
            )
            copies[-1].start()
    qs_ref[0] = qt_ref[...]
    hs_ref[0] = h_ref[...]
    for copy in copies:
        copy.wait()
    for d in range(1, n):
        qs_ref[d] = qland[d - 1]
        hs_ref[d] = hland[d - 1]


def second_kernel(n, qs_ref, hs_ref, st_ref, zt_ref, rows_ref):
    st = st_ref[...]
    m, cols = st.shape
    qs = qs_ref[...].reshape(n * m, cols)
    us = dot(st, qs, 1, 1)
    vs = jnp.concatenate([dot(us[:, g * m : g * m + m], hs_ref[g]) for g in range(n)], axis=1)
    q2 = orthonormal(dot(vs, qs), rows_ref)
    u = dot(st, q2, 1, 1)
    s = dot(q2, qs, 1, 1)
    w = dot(u, s)
    w = jnp.concatenate([dot(w[:, g * m : g * m + m], hs_ref[g]) for g in range(n)], axis=1)
    zt_ref[...] = dot(dot(w, s, 1, 1), q2)


def sum_kernel(n, z_ref, y_ref, mine, land, reduced, gathered, rs_send, rs_recv, ag_send, ag_recv):
    entry_barrier([("leaf", n)])
    me = lax.axis_index("leaf")

    def exchange(d, source, target, ss, rs):
        peer = lax.rem(me + d, n)
        return pltpu.make_async_remote_copy(
            src_ref=source(peer), dst_ref=target.at[d - 1], send_sem=ss.at[d - 1], recv_sem=rs.at[d - 1],
            device_id={"leaf": peer}, device_id_type=MESH,
        )

    scatter = [exchange(d, lambda p: z_ref.at[p], land, rs_send, rs_recv) for d in range(1, n)]
    for copy in scatter:
        copy.start()
    total = z_ref[me]
    for d, copy in enumerate(scatter):
        copy.wait_recv()
        total = total + land[d]
    reduced[...] = total
    gather = [exchange(d, lambda p: reduced, gathered, ag_send, ag_recv) for d in range(1, n)]
    for copy in gather:
        copy.start()
    y_ref[me] = total
    for copy in scatter:
        copy.wait_send()
    for d in range(1, n):
        gather[d - 1].wait()
        y_ref[lax.rem(me + n - d, n)] = gathered[d - 1]


def project_kernel(x_hbm, yt_ref, o_hbm, xbuf, obuf, phi, pmid, rows_ref, sems, osems):
    chunks = x_hbm.shape[0] // CHUNK

    def copy(i):
        at = pl.ds(pl.multiple_of(i * CHUNK, CHUNK), CHUNK)
        return pltpu.make_async_copy(x_hbm.at[at], xbuf.at[at], sems.at[i])

    def out(i):
        at = pl.ds(pl.multiple_of(i * CHUNK, CHUNK), CHUNK)
        return pltpu.make_async_copy(obuf.at[at], o_hbm.at[at], osems.at[i])

    for i in range(chunks):
        copy(i).start()
    qt = orthonormal(yt_ref[...], rows_ref)
    hi, mid = split(dot(qt, qt, 0, 0))
    phi[...] = hi
    pmid[...] = mid

    def step(i, carry):
        copy(i).wait()
        at = pl.ds(pl.multiple_of(i * CHUNK, CHUNK), CHUNK)
        hi, mid = split(xbuf[at, :])
        obuf[at, :] = (fast(hi, phi[...]) + (fast(hi, pmid[...]) + fast(mid, phi[...]))).astype(jnp.bfloat16)
        out(i).start()
        return carry

    lax.fori_loop(0, chunks, step, 0)
    for i in range(chunks):
        out(i).wait()


def local(n_grp, n_leaf, x, sketch):
    rows, cols = x.shape
    modes = sketch.shape[1]
    chunks = rows // CHUNK
    f32 = jnp.float32
    hbm = pl.BlockSpec(memory_space=pl.ANY)
    st = sketch.T
    dma = pltpu.SemaphoreType.DMA
    qt, h = pl.pallas_call(
        first_kernel,
        out_shape=(jax.ShapeDtypeStruct((modes, cols), f32), jax.ShapeDtypeStruct((modes, modes), f32)),
        in_specs=[hbm, VMEM],
        out_specs=(VMEM, VMEM),
        scratch_shapes=[
            pltpu.VMEM((rows, cols), f32), pltpu.VMEM((cols, 2 * cols), f32), pltpu.VMEM((cols, cols), f32),
            pltpu.VMEM((modes, 2 * modes), f32), dma((chunks,)),
        ],
    )(x, st)
    qs, hs = pl.pallas_call(
        functools.partial(group_kernel, n_grp),
        out_shape=(jax.ShapeDtypeStruct((n_grp, modes, cols), f32), jax.ShapeDtypeStruct((n_grp, modes, modes), f32)),
        in_specs=[VMEM, VMEM],
        out_specs=(VMEM, VMEM),
        scratch_shapes=[
            pltpu.VMEM((n_grp - 1, modes, cols), f32), pltpu.VMEM((n_grp - 1, modes, modes), f32),
            dma((n_grp - 1,)), dma((n_grp - 1,)), dma((n_grp - 1,)), dma((n_grp - 1,)),
        ],
        compiler_params=pltpu.CompilerParams(collective_id=0, has_side_effects=True),
    )(qt, h)
    zt = pl.pallas_call(
        functools.partial(second_kernel, n_grp),
        out_shape=jax.ShapeDtypeStruct((modes, cols), f32),
        in_specs=[VMEM] * 3,
        out_specs=VMEM,
        scratch_shapes=[pltpu.VMEM((modes, 2 * modes), f32)],
    )(qs, hs, st)
    piece = (modes * cols // (n_leaf * LANES), LANES)
    wide = cols // LANES
    z = jnp.concatenate([zt[:, LANES * i : LANES * i + LANES] for i in range(wide)], axis=0).reshape(n_leaf, *piece)
    y = pl.pallas_call(
        functools.partial(sum_kernel, n_leaf),
        out_shape=jax.ShapeDtypeStruct((n_leaf, *piece), f32),
        in_specs=[VMEM],
        out_specs=VMEM,
        scratch_shapes=[
            pltpu.VMEM(piece, f32), pltpu.VMEM((n_leaf - 1, *piece), f32), pltpu.VMEM(piece, f32),
            pltpu.VMEM((n_leaf - 1, *piece), f32),
            dma((n_leaf - 1,)), dma((n_leaf - 1,)), dma((n_leaf - 1,)), dma((n_leaf - 1,)),
        ],
        compiler_params=pltpu.CompilerParams(collective_id=1, has_side_effects=True),
    )(z)
    y = y.reshape(wide * modes, LANES)
    yt = jnp.concatenate([y[modes * i : modes * i + modes] for i in range(wide)], axis=1)
    return pl.pallas_call(
        project_kernel,
        out_shape=jax.ShapeDtypeStruct((rows, cols), jnp.bfloat16),
        in_specs=[hbm, VMEM],
        out_specs=hbm,
        scratch_shapes=[
            pltpu.VMEM((rows, cols), f32), pltpu.VMEM((rows, cols), jnp.bfloat16),
            pltpu.VMEM((cols, cols), jnp.bfloat16), pltpu.VMEM((cols, cols), jnp.bfloat16),
            pltpu.VMEM((modes, 2 * modes), f32), dma((chunks,)), dma((chunks,)),
        ],
    )(x, yt)


def solution(mesh):
    return jax.shard_map(
        functools.partial(local, mesh.shape["grp"], mesh.shape["leaf"]),
        mesh=mesh,
        in_specs=(P(("grp", "leaf"), None), P()),
        out_specs=P(("grp", "leaf"), None),
        check_vma=False,
    )
```

```python
import functools

import jax
import jax.numpy as jnp
from jax import lax
from jax.experimental import pallas as pl
from jax.experimental.pallas import tpu as pltpu
from jax.sharding import PartitionSpec as P

MESH = pl.DeviceIdType.MESH
VMEM = pl.BlockSpec(memory_space=pltpu.VMEM)
LANES = 128
CHUNK = 512


def dot(a, b, ca=1, cb=0):
    return lax.dot_general(
        a, b, (((ca,), (cb,)), ((), ())),
        precision=lax.Precision.HIGHEST, preferred_element_type=jnp.float32,
    )


def fast(a, b, ca=1, cb=0):
    return lax.dot_general(a, b, (((ca,), (cb,)), ((), ())), preferred_element_type=jnp.float32)


def split(x):
    hi = x.astype(jnp.bfloat16)
    return hi, (x - hi.astype(jnp.float32)).astype(jnp.bfloat16)


def three(a, b):
    (ah, am), (bh, bm) = split(a), split(b)
    return fast(ah, bh) + (fast(ah, bm) + fast(am, bh))


def identity(n):
    return (lax.broadcasted_iota(jnp.int32, (n, n), 0) == lax.broadcasted_iota(jnp.int32, (n, n), 1)).astype(jnp.float32)


def inverse_factor(c, rows_ref):
    m = c.shape[0]
    full = jnp.concatenate([c, identity(m)], axis=1)
    width = 2 * m
    blocks = [full[8 * k : 8 * k + 8] for k in range(m // 8)]
    for j in range(0, m, 2):
        k, s = j // 8, j % 8
        lead = blocks[k]
        cols = [
            (
                jnp.broadcast_to(blocks[i][:, j : j + 1], (8, width)),
                jnp.broadcast_to(blocks[i][:, j + 1 : j + 2], (8, width)),
            )
            for i in range(k, m // 8)
        ]
        r0, r1 = lead[s : s + 1], lead[s + 1 : s + 2]
        a, b, d = cols[0][0][s : s + 1], cols[0][0][s + 1 : s + 2], cols[0][1][s + 1 : s + 2]
        det = a * d - b * b
        inv = 1.0 / det
        t0 = (d * r0 - b * r1) * inv
        t1 = (a * r1 - b * r0) * inv
        for i in range(k, m // 8):
            c0, c1 = cols[i - k]
            blocks[i] = blocks[i] - c0 * t0 - c1 * t1
        ia = lax.rsqrt(a)
        rows_ref[j : j + 1, :] = r0 * ia
        rows_ref[j + 1 : j + 2, :] = (a * r1 - b * r0) * (ia * lax.rsqrt(det))
    return rows_ref[:, m:]


def orthonormal(yt, rows_ref):
    m = yt.shape[0]
    qt = dot(inverse_factor(dot(yt, yt, 1, 1), rows_ref), yt)
    err = identity(m) - dot(qt, qt, 1, 1)
    near = err.astype(jnp.bfloat16)
    fix = 0.5 * err + 0.375 * fast(near, near)
    return qt + three(fix, qt)


def merge_kernel(n_grp, n_leaf, x_hbm, st_ref, yt_ref, xbuf, acc, acc2, rows_ref, qall, hall, z, land, total, yall, sems, qsem, hsem, rsem, gsem):
    chunks = x_hbm.shape[0] // CHUNK
    m, cols = st_ref.shape
    grp, leaf = lax.axis_index("grp"), lax.axis_index("leaf")

    def copy(i):
        at = pl.ds(pl.multiple_of(i * CHUNK, CHUNK), CHUNK)
        return pltpu.make_async_copy(x_hbm.at[at], xbuf.at[at], sems.at[i])

    for i in range(chunks):
        copy(i).start()
    barrier = pltpu.get_barrier_semaphore()
    for axis, me, n in (("grp", grp, n_grp), ("leaf", leaf, n_leaf)):
        for d in range(1, n):
            pl.semaphore_signal(barrier, inc=1, device_id={axis: lax.rem(me + d, n)}, device_id_type=MESH)

    acc[...] = jnp.zeros_like(acc)
    acc2[...] = jnp.zeros_like(acc2)

    def step(i, carry):
        copy(i).wait()
        hi, mid = split(xbuf[pl.ds(pl.multiple_of(i * CHUNK, CHUNK), CHUNK), :])
        acc[...] += fast(hi, jnp.concatenate([hi, mid], axis=1), 0, 0)
        acc2[...] += fast(mid, mid, 0, 0)
        return carry

    lax.fori_loop(0, chunks, step, 0)
    cross = acc[:, cols:]
    gram = acc[:, :cols] + (cross + cross.T + acc2[...])
    qt = orthonormal(dot(st_ref[...], gram), rows_ref)
    qall[0] = qt
    pl.semaphore_wait(barrier, n_grp + n_leaf - 2)

    def send(src, dst, sem, d, axis, me, n):
        return pltpu.make_async_remote_copy(
            src_ref=src, dst_ref=dst, send_sem=sem.at[0, d - 1], recv_sem=sem.at[1, d - 1],
            device_id={axis: lax.rem(me + d, n)}, device_id_type=MESH,
        )

    to_group = [send(qall.at[0], qall.at[d], qsem, d, "grp", grp, n_grp) for d in range(1, n_grp)]
    for c in to_group:
        c.start()
    hall[0] = dot(dot(qt, gram), qt, 1, 1)
    to_group_h = [send(hall.at[0], hall.at[d], hsem, d, "grp", grp, n_grp) for d in range(1, n_grp)]
    for c in to_group_h:
        c.start()
    for c in to_group:
        c.wait()
    st = st_ref[...]
    qs = qall[...].reshape(n_grp * m, cols)
    us = dot(st, qs, 1, 1)
    for c in to_group_h:
        c.wait()
    vs = jnp.concatenate([dot(us[:, g * m : g * m + m], hall[g]) for g in range(n_grp)], axis=1)
    q2 = orthonormal(dot(vs, qs), rows_ref)
    u = dot(st, q2, 1, 1)
    s = dot(q2, qs, 1, 1)
    w = dot(u, s)
    w = jnp.concatenate([dot(w[:, g * m : g * m + m], hall[g]) for g in range(n_grp)], axis=1)
    zt = dot(dot(w, s, 1, 1), q2)

    rows = z.shape[1]
    for p in range(n_leaf):
        at, wide = (p * rows) % m, (p * rows) // m * LANES
        z[p] = zt[at : at + rows, wide : wide + LANES]
    scatter = [send(z.at[lax.rem(leaf + d, n_leaf)], land.at[d - 1], rsem, d, "leaf", leaf, n_leaf) for d in range(1, n_leaf)]
    for c in scatter:
        c.start()
    part = z[leaf]
    for d, c in enumerate(scatter):
        c.wait_recv()
        part = part + land[d]
    total[...] = part
    gather = [send(total, yall.at[leaf], gsem, d, "leaf", leaf, n_leaf) for d in range(1, n_leaf)]
    for c in gather:
        c.start()
    yall[leaf] = part
    for c in scatter:
        c.wait_send()
    for c in gather:
        c.wait()
    for p in range(n_leaf):
        at, wide = (p * rows) % m, (p * rows) // m * LANES
        yt_ref[at : at + rows, wide : wide + LANES] = yall[p]


def project_kernel(x_hbm, yt_ref, o_hbm, xbuf, obuf, phi, pmid, rows_ref, sems, osems):
    chunks = x_hbm.shape[0] // CHUNK

    def copy(i):
        at = pl.ds(pl.multiple_of(i * CHUNK, CHUNK), CHUNK)
        return pltpu.make_async_copy(x_hbm.at[at], xbuf.at[at], sems.at[i])

    def out(i):
        at = pl.ds(pl.multiple_of(i * CHUNK, CHUNK), CHUNK)
        return pltpu.make_async_copy(obuf.at[at], o_hbm.at[at], osems.at[i])

    for i in range(chunks):
        copy(i).start()
    qt = orthonormal(yt_ref[...], rows_ref)
    hi, mid = split(dot(qt, qt, 0, 0))
    phi[...] = hi
    pmid[...] = mid

    def step(i, carry):
        copy(i).wait()
        at = pl.ds(pl.multiple_of(i * CHUNK, CHUNK), CHUNK)
        hi, mid = split(xbuf[at, :])
        obuf[at, :] = (fast(hi, phi[...]) + (fast(hi, pmid[...]) + fast(mid, phi[...]))).astype(jnp.bfloat16)
        out(i).start()
        return carry

    lax.fori_loop(0, chunks, step, 0)
    for i in range(chunks):
        out(i).wait()


def local(n_grp, n_leaf, x, sketch):
    rows, cols = x.shape
    modes = sketch.shape[1]
    chunks = rows // CHUNK
    f32 = jnp.float32
    hbm = pl.BlockSpec(memory_space=pl.ANY)
    dma = pltpu.SemaphoreType.DMA
    piece = (modes * cols // (n_leaf * LANES), LANES)
    yt = pl.pallas_call(
        functools.partial(merge_kernel, n_grp, n_leaf),
        out_shape=jax.ShapeDtypeStruct((modes, cols), f32),
        in_specs=[hbm, VMEM],
        out_specs=VMEM,
        scratch_shapes=[
            pltpu.VMEM((rows, cols), f32), pltpu.VMEM((cols, 2 * cols), f32), pltpu.VMEM((cols, cols), f32),
            pltpu.VMEM((modes, 2 * modes), f32),
            pltpu.VMEM((n_grp, modes, cols), f32), pltpu.VMEM((n_grp, modes, modes), f32),
            pltpu.VMEM((n_leaf, *piece), f32), pltpu.VMEM((n_leaf - 1, *piece), f32),
            pltpu.VMEM(piece, f32), pltpu.VMEM((n_leaf, *piece), f32),
            dma((chunks,)), dma((2, n_grp - 1)), dma((2, n_grp - 1)), dma((2, n_leaf - 1)), dma((2, n_leaf - 1)),
        ],
        compiler_params=pltpu.CompilerParams(collective_id=0, has_side_effects=True),
    )(x, sketch.T)
    return pl.pallas_call(
        project_kernel,
        out_shape=jax.ShapeDtypeStruct((rows, cols), jnp.bfloat16),
        in_specs=[hbm, VMEM],
        out_specs=hbm,
        scratch_shapes=[
            pltpu.VMEM((rows, cols), f32), pltpu.VMEM((rows, cols), jnp.bfloat16),
            pltpu.VMEM((cols, cols), jnp.bfloat16), pltpu.VMEM((cols, cols), jnp.bfloat16),
            pltpu.VMEM((modes, 2 * modes), f32), dma((chunks,)), dma((chunks,)),
        ],
    )(x, yt)


def solution(mesh):
    return jax.shard_map(
        functools.partial(local, mesh.shape["grp"], mesh.shape["leaf"]),
        mesh=mesh,
        in_specs=(P(("grp", "leaf"), None), P()),
        out_specs=P(("grp", "leaf"), None),
        check_vma=False,
    )
```

```python
import functools

import jax
import jax.numpy as jnp
from jax import lax
from jax.experimental import pallas as pl
from jax.experimental.pallas import tpu as pltpu
from jax.sharding import PartitionSpec as P

MESH = pl.DeviceIdType.MESH
VMEM = pl.BlockSpec(memory_space=pltpu.VMEM)
LANES = 128
CHUNK = 512


def dot(a, b, ca=1, cb=0):
    return lax.dot_general(
        a, b, (((ca,), (cb,)), ((), ())),
        precision=lax.Precision.HIGHEST, preferred_element_type=jnp.float32,
    )


def fast(a, b, ca=1, cb=0):
    return lax.dot_general(a, b, (((ca,), (cb,)), ((), ())), preferred_element_type=jnp.float32)


def split(x):
    hi = x.astype(jnp.bfloat16)
    return hi, (x - hi.astype(jnp.float32)).astype(jnp.bfloat16)


def three(a, b):
    (ah, am), (bh, bm) = split(a), split(b)
    return fast(ah, bh) + (fast(ah, bm) + fast(am, bh))


def identity(n):
    return (lax.broadcasted_iota(jnp.int32, (n, n), 0) == lax.broadcasted_iota(jnp.int32, (n, n), 1)).astype(jnp.float32)


def eliminate(s, rhs, emit):
    b = len(s)
    if b == 2:
        det = s[0][0] * s[1][1] - s[1][0] * s[1][0]
        inv = 1.0 / det
        low = [s[0][0] * r[1] - s[1][0] * r[0] for r in rhs]
        if emit is not None:
            scale = lax.rsqrt(s[0][0])
            emit(rhs[0][0] * scale)
            emit(low[0] * (scale * lax.rsqrt(det)))
        return [[(s[1][1] * r[0] - s[1][0] * r[1]) * inv, l * inv] for r, l in zip(rhs, low)]
    h = b // 2
    side = [[s[h + p][q] for q in range(h)] for p in range(h)]
    upper = [[s[p][q] if q <= p else s[q][p] for q in range(h)] for p in range(h)]
    done = eliminate(upper, [r[:h] for r in rhs] + side, emit)
    tops, u = done[: len(rhs)], done[len(rhs) :]

    def apply(row, vector):
        terms = [row[q] * vector[q] for q in range(h)]
        while len(terms) > 1:
            terms = [x + y for x, y in zip(terms[::2], terms[1::2])]
        return terms[0]

    schur = [[s[h + p][h + q] - apply(side[p], u[q]) if q <= p else None for q in range(h)] for p in range(h)]
    rest = [[r[h + p] - apply(side[p], t) for p in range(h)] for r, t in zip(rhs, tops)]
    bottoms = eliminate(schur, rest, emit)
    return [
        [t[p] - apply([u[q][p] for q in range(h)], v) for p in range(h)] + v for t, v in zip(tops, bottoms)
    ]


def inverse_factor(c, rows_ref, b=8):
    m = c.shape[0]
    full = jnp.concatenate([c, identity(m)], axis=1)
    tile = (8, 2 * m)
    blocks = [full[8 * k : 8 * k + 8] for k in range(m // 8)]
    for j in range(0, m, b):
        k, at = j // 8, j % 8
        cols = [[jnp.broadcast_to(blocks[i][:, j + q : j + q + 1], tile) for q in range(b)] for i in range(k, m // 8)]
        rows = [jnp.broadcast_to(blocks[k][at + p : at + p + 1], tile) for p in range(b)]
        pivot = [[jnp.broadcast_to(cols[0][q][at + p : at + p + 1], tile) if q <= p else None for q in range(b)] for p in range(b)]
        place = [j]

        def emit(row):
            rows_ref[place[0] : place[0] + 1, :] = row[:1]
            place[0] += 1

        (t,) = eliminate(pivot, [rows], emit)
        for i in range(k if at + b < 8 else k + 1, m // 8):
            terms = [x * y for x, y in zip(cols[i - k], t)]
            while len(terms) > 1:
                terms = [x + y for x, y in zip(terms[::2], terms[1::2])]
            blocks[i] = blocks[i] - terms[0]
    return rows_ref[:, m:]


def orthonormal(yt, rows_ref):
    m = yt.shape[0]
    qt = dot(inverse_factor(dot(yt, yt, 1, 1), rows_ref), yt)
    err = identity(m) - dot(qt, qt, 1, 1)
    near = err.astype(jnp.bfloat16)
    fix = 0.5 * err + 0.375 * fast(near, near)
    return qt + three(fix, qt)


def merge_kernel(n_grp, n_leaf, x_hbm, st_ref, yt_ref, xbuf, acc, acc2, rows_ref, qall, hall, z, land, total, yall, sems, qsem, hsem, rsem, gsem):
    chunks = x_hbm.shape[0] // CHUNK
    m, cols = st_ref.shape
    grp, leaf = lax.axis_index("grp"), lax.axis_index("leaf")

    def copy(i):
        at = pl.ds(pl.multiple_of(i * CHUNK, CHUNK), CHUNK)
        return pltpu.make_async_copy(x_hbm.at[at], xbuf.at[at], sems.at[i])

    for i in range(chunks):
        copy(i).start()
    barrier = pltpu.get_barrier_semaphore()
    for axis, me, n in (("grp", grp, n_grp), ("leaf", leaf, n_leaf)):
        for d in range(1, n):
            pl.semaphore_signal(barrier, inc=1, device_id={axis: lax.rem(me + d, n)}, device_id_type=MESH)

    acc[...] = jnp.zeros_like(acc)
    acc2[...] = jnp.zeros_like(acc2)

    def step(i, carry):
        copy(i).wait()
        hi, mid = split(xbuf[pl.ds(pl.multiple_of(i * CHUNK, CHUNK), CHUNK), :])
        acc[...] += fast(hi, jnp.concatenate([hi, mid], axis=1), 0, 0)
        acc2[...] += fast(mid, mid, 0, 0)
        return carry

    lax.fori_loop(0, chunks, step, 0)
    cross = acc[:, cols:]
    gram = acc[:, :cols] + (cross + cross.T + acc2[...])
    qt = orthonormal(dot(st_ref[...], gram), rows_ref)
    qall[0] = qt
    pl.semaphore_wait(barrier, n_grp + n_leaf - 2)

    def send(src, dst, sem, d, axis, me, n):
        return pltpu.make_async_remote_copy(
            src_ref=src, dst_ref=dst, send_sem=sem.at[0, d - 1], recv_sem=sem.at[1, d - 1],
            device_id={axis: lax.rem(me + d, n)}, device_id_type=MESH,
        )

    to_group = [send(qall.at[0], qall.at[d], qsem, d, "grp", grp, n_grp) for d in range(1, n_grp)]
    for c in to_group:
        c.start()
    hall[0] = dot(dot(qt, gram), qt, 1, 1)
    to_group_h = [send(hall.at[0], hall.at[d], hsem, d, "grp", grp, n_grp) for d in range(1, n_grp)]
    for c in to_group_h:
        c.start()
    for c in to_group:
        c.wait()
    st = st_ref[...]
    qs = qall[...].reshape(n_grp * m, cols)
    for c in to_group_h:
        c.wait()
    ts = jnp.concatenate([dot(hall[g], qs[g * m : g * m + m]) for g in range(n_grp)], axis=0)
    pair_gram = dot(qs, ts, 0, 0)
    q2 = orthonormal(dot(st, pair_gram), rows_ref)
    h2 = dot(dot(q2, pair_gram), q2, 1, 1)
    zt = dot(dot(dot(st, q2, 1, 1), h2), q2)

    rows = z.shape[1]
    for p in range(n_leaf):
        at, wide = (p * rows) % m, (p * rows) // m * LANES
        z[p] = zt[at : at + rows, wide : wide + LANES]
    scatter = [send(z.at[lax.rem(leaf + d, n_leaf)], land.at[d - 1], rsem, d, "leaf", leaf, n_leaf) for d in range(1, n_leaf)]
    for c in scatter:
        c.start()
    part = z[leaf]
    for d, c in enumerate(scatter):
        c.wait_recv()
        part = part + land[d]
    total[...] = part
    gather = [send(total, yall.at[leaf], gsem, d, "leaf", leaf, n_leaf) for d in range(1, n_leaf)]
    for c in gather:
        c.start()
    yall[leaf] = part
    for c in scatter:
        c.wait_send()
    for c in gather:
        c.wait()
    for p in range(n_leaf):
        at, wide = (p * rows) % m, (p * rows) // m * LANES
        yt_ref[at : at + rows, wide : wide + LANES] = yall[p]


def project_kernel(x_hbm, yt_ref, o_hbm, xbuf, obuf, proj, rows_ref, sems, osems):
    chunks = x_hbm.shape[0] // CHUNK

    def copy(i):
        at = pl.ds(pl.multiple_of(i * CHUNK, CHUNK), CHUNK)
        return pltpu.make_async_copy(x_hbm.at[at], xbuf.at[at], sems.at[i])

    def out(i):
        at = pl.ds(pl.multiple_of(i * CHUNK, CHUNK), CHUNK)
        return pltpu.make_async_copy(obuf.at[at], o_hbm.at[at], osems.at[i])

    for i in range(chunks):
        copy(i).start()
    qt = orthonormal(yt_ref[...], rows_ref)
    hi, mid = split(dot(qt, qt, 0, 0))
    proj[...] = jnp.concatenate([hi, mid, hi], axis=0)

    def step(i, carry):
        copy(i).wait()
        at = pl.ds(pl.multiple_of(i * CHUNK, CHUNK), CHUNK)
        hi, mid = split(xbuf[at, :])
        obuf[at, :] = fast(jnp.concatenate([hi, hi, mid], axis=1), proj[...]).astype(jnp.bfloat16)
        out(i).start()
        return carry

    lax.fori_loop(0, chunks, step, 0)
    for i in range(chunks):
        out(i).wait()


def local(n_grp, n_leaf, x, sketch):
    rows, cols = x.shape
    modes = sketch.shape[1]
    chunks = rows // CHUNK
    f32 = jnp.float32
    hbm = pl.BlockSpec(memory_space=pl.ANY)
    dma = pltpu.SemaphoreType.DMA
    piece = (modes * cols // (n_leaf * LANES), LANES)
    yt = pl.pallas_call(
        functools.partial(merge_kernel, n_grp, n_leaf),
        out_shape=jax.ShapeDtypeStruct((modes, cols), f32),
        in_specs=[hbm, VMEM],
        out_specs=VMEM,
        scratch_shapes=[
            pltpu.VMEM((rows, cols), f32), pltpu.VMEM((cols, 2 * cols), f32), pltpu.VMEM((cols, cols), f32),
            pltpu.VMEM((modes, 2 * modes), f32),
            pltpu.VMEM((n_grp, modes, cols), f32), pltpu.VMEM((n_grp, modes, modes), f32),
            pltpu.VMEM((n_leaf, *piece), f32), pltpu.VMEM((n_leaf - 1, *piece), f32),
            pltpu.VMEM(piece, f32), pltpu.VMEM((n_leaf, *piece), f32),
            dma((chunks,)), dma((2, n_grp - 1)), dma((2, n_grp - 1)), dma((2, n_leaf - 1)), dma((2, n_leaf - 1)),
        ],
        compiler_params=pltpu.CompilerParams(collective_id=0, has_side_effects=True),
    )(x, sketch.T)
    return pl.pallas_call(
        project_kernel,
        out_shape=jax.ShapeDtypeStruct((rows, cols), jnp.bfloat16),
        in_specs=[hbm, VMEM],
        out_specs=hbm,
        scratch_shapes=[
            pltpu.VMEM((rows, cols), f32), pltpu.VMEM((rows, cols), jnp.bfloat16),
            pltpu.VMEM((3 * cols, cols), jnp.bfloat16),
            pltpu.VMEM((modes, 2 * modes), f32), dma((chunks,)), dma((chunks,)),
        ],
    )(x, yt)


def solution(mesh):
    return jax.shard_map(
        functools.partial(local, mesh.shape["grp"], mesh.shape["leaf"]),
        mesh=mesh,
        in_specs=(P(("grp", "leaf"), None), P()),
        out_specs=P(("grp", "leaf"), None),
        check_vma=False,
    )
```

```python
import functools

import jax
import jax.numpy as jnp
from jax import lax
from jax.experimental import pallas as pl
from jax.experimental.pallas import tpu as pltpu
from jax.sharding import PartitionSpec as P

MESH = pl.DeviceIdType.MESH
VMEM = pl.BlockSpec(memory_space=pltpu.VMEM)
LANES = 128
CHUNK = 1024


def dot(a, b, ca=1, cb=0):
    return lax.dot_general(
        a, b, (((ca,), (cb,)), ((), ())),
        precision=lax.Precision.HIGHEST, preferred_element_type=jnp.float32,
    )


def fast(a, b, ca=1, cb=0):
    return lax.dot_general(a, b, (((ca,), (cb,)), ((), ())), preferred_element_type=jnp.float32)


def split(x):
    hi = x.astype(jnp.bfloat16)
    return hi, (x - hi.astype(jnp.float32)).astype(jnp.bfloat16)


def three(a, b):
    (ah, am), (bh, bm) = split(a), split(b)
    return fast(ah, bh) + (fast(ah, bm) + fast(am, bh))


def identity(n):
    return (lax.broadcasted_iota(jnp.int32, (n, n), 0) == lax.broadcasted_iota(jnp.int32, (n, n), 1)).astype(jnp.float32)


def eliminate(s, rhs, emit):
    b = len(s)
    if b == 2:
        det = s[0][0] * s[1][1] - s[1][0] * s[1][0]
        inv = 1.0 / det
        low = [s[0][0] * r[1] - s[1][0] * r[0] for r in rhs]
        if emit is not None:
            scale = lax.rsqrt(s[0][0])
            emit(rhs[0][0] * scale)
            emit(low[0] * (scale * lax.rsqrt(det)))
        return [[(s[1][1] * r[0] - s[1][0] * r[1]) * inv, l * inv] for r, l in zip(rhs, low)]
    h = b // 2
    side = [[s[h + p][q] for q in range(h)] for p in range(h)]
    upper = [[s[p][q] if q <= p else s[q][p] for q in range(h)] for p in range(h)]
    done = eliminate(upper, [r[:h] for r in rhs] + side, emit)
    tops, u = done[: len(rhs)], done[len(rhs) :]

    def apply(row, vector):
        terms = [row[q] * vector[q] for q in range(h)]
        while len(terms) > 1:
            terms = [x + y for x, y in zip(terms[::2], terms[1::2])]
        return terms[0]

    schur = [[s[h + p][h + q] - apply(side[p], u[q]) if q <= p else None for q in range(h)] for p in range(h)]
    rest = [[r[h + p] - apply(side[p], t) for p in range(h)] for r, t in zip(rhs, tops)]
    bottoms = eliminate(schur, rest, emit)
    return [
        [t[p] - apply([u[q][p] for q in range(h)], v) for p in range(h)] + v for t, v in zip(tops, bottoms)
    ]


def inverse_factor(c, rows_ref, b=8):
    m = c.shape[0]
    full = jnp.concatenate([c, identity(m)], axis=1)
    tile = (8, 2 * m)
    blocks = [full[8 * k : 8 * k + 8] for k in range(m // 8)]
    for j in range(0, m, b):
        k, at = j // 8, j % 8
        cols = [[jnp.broadcast_to(blocks[i][:, j + q : j + q + 1], tile) for q in range(b)] for i in range(k, m // 8)]
        rows = [jnp.broadcast_to(blocks[k][at + p : at + p + 1], tile) for p in range(b)]
        pivot = [[jnp.broadcast_to(cols[0][q][at + p : at + p + 1], tile) if q <= p else None for q in range(b)] for p in range(b)]
        place = [j]

        def emit(row):
            rows_ref[place[0] : place[0] + 1, :] = row[:1]
            place[0] += 1

        (t,) = eliminate(pivot, [rows], emit)
        for i in range(k if at + b < 8 else k + 1, m // 8):
            terms = [x * y for x, y in zip(cols[i - k], t)]
            while len(terms) > 1:
                terms = [x + y for x, y in zip(terms[::2], terms[1::2])]
            blocks[i] = blocks[i] - terms[0]
    return rows_ref[:, m:]


def orthonormal(yt, rows_ref):
    m = yt.shape[0]
    qt = dot(inverse_factor(dot(yt, yt, 1, 1), rows_ref), yt)
    err = identity(m) - dot(qt, qt, 1, 1)
    near = err.astype(jnp.bfloat16)
    fix = 0.5 * err + 0.375 * fast(near, near)
    return qt + three(fix, qt)


def merge_kernel(n_grp, n_leaf, x_hbm, st_ref, yt_ref, xbuf, acc, acc2, rows_ref, qall, hall, z, land, total, yall, sems, qsem, hsem, rsem, gsem):
    chunks = x_hbm.shape[0] // CHUNK
    m, cols = st_ref.shape
    grp, leaf = lax.axis_index("grp"), lax.axis_index("leaf")

    def copy(i):
        at = pl.ds(pl.multiple_of(i * CHUNK, CHUNK), CHUNK)
        return pltpu.make_async_copy(x_hbm.at[at], xbuf.at[at], sems.at[i])

    for i in range(chunks):
        copy(i).start()
    barrier = pltpu.get_barrier_semaphore()
    for axis, me, n in (("grp", grp, n_grp), ("leaf", leaf, n_leaf)):
        for d in range(1, n):
            pl.semaphore_signal(barrier, inc=1, device_id={axis: lax.rem(me + d, n)}, device_id_type=MESH)

    acc[...] = jnp.zeros_like(acc)
    acc2[...] = jnp.zeros_like(acc2)

    def step(i, carry):
        copy(i).wait()
        hi, mid = split(xbuf[pl.ds(pl.multiple_of(i * CHUNK, CHUNK), CHUNK), :])
        acc[...] += fast(hi, jnp.concatenate([hi, mid], axis=1), 0, 0)
        acc2[...] += fast(mid, mid, 0, 0)
        return carry

    lax.fori_loop(0, chunks, step, 0)
    cross = acc[:, cols:]
    gram = acc[:, :cols] + (cross + cross.T + acc2[...])
    qt = orthonormal(dot(st_ref[...], gram), rows_ref)
    qall[0] = qt
    pl.semaphore_wait(barrier, n_grp + n_leaf - 2)

    def send(src, dst, sem, d, axis, me, n):
        return pltpu.make_async_remote_copy(
            src_ref=src, dst_ref=dst, send_sem=sem.at[0, d - 1], recv_sem=sem.at[1, d - 1],
            device_id={axis: lax.rem(me + d, n)}, device_id_type=MESH,
        )

    to_group = [send(qall.at[0], qall.at[d], qsem, d, "grp", grp, n_grp) for d in range(1, n_grp)]
    for c in to_group:
        c.start()
    hall[0] = dot(dot(qt, gram), qt, 1, 1)
    to_group_h = [send(hall.at[0], hall.at[d], hsem, d, "grp", grp, n_grp) for d in range(1, n_grp)]
    for c in to_group_h:
        c.start()
    for c in to_group:
        c.wait()
    st = st_ref[...]
    qs = qall[...].reshape(n_grp * m, cols)
    for c in to_group_h:
        c.wait()
    ts = jnp.concatenate([dot(hall[g], qs[g * m : g * m + m]) for g in range(n_grp)], axis=0)
    pair_gram = dot(qs, ts, 0, 0)
    q2 = orthonormal(dot(st, pair_gram), rows_ref)
    h2 = dot(dot(q2, pair_gram), q2, 1, 1)
    zt = dot(dot(dot(st, q2, 1, 1), h2), q2)

    rows = z.shape[1]
    for p in range(n_leaf):
        at, wide = (p * rows) % m, (p * rows) // m * LANES
        z[p] = zt[at : at + rows, wide : wide + LANES]
    scatter = [send(z.at[lax.rem(leaf + d, n_leaf)], land.at[d - 1], rsem, d, "leaf", leaf, n_leaf) for d in range(1, n_leaf)]
    for c in scatter:
        c.start()
    part = z[leaf]
    for d, c in enumerate(scatter):
        c.wait_recv()
        part = part + land[d]
    total[...] = part
    gather = [send(total, yall.at[leaf], gsem, d, "leaf", leaf, n_leaf) for d in range(1, n_leaf)]
    for c in gather:
        c.start()
    yall[leaf] = part
    for c in scatter:
        c.wait_send()
    for c in gather:
        c.wait()
    for p in range(n_leaf):
        at, wide = (p * rows) % m, (p * rows) // m * LANES
        yt_ref[at : at + rows, wide : wide + LANES] = yall[p]


def project_kernel(x_hbm, yt_ref, o_hbm, xbuf, obuf, proj, rows_ref, sems, osems):
    chunks = x_hbm.shape[0] // CHUNK

    def copy(i):
        at = pl.ds(pl.multiple_of(i * CHUNK, CHUNK), CHUNK)
        return pltpu.make_async_copy(x_hbm.at[at], xbuf.at[at], sems.at[i])

    def out(i):
        at = pl.ds(pl.multiple_of(i * CHUNK, CHUNK), CHUNK)
        return pltpu.make_async_copy(obuf.at[at], o_hbm.at[at], osems.at[i])

    for i in range(chunks):
        copy(i).start()
    qt = orthonormal(yt_ref[...], rows_ref)
    hi, mid = split(dot(qt, qt, 0, 0))
    proj[...] = jnp.concatenate([hi, mid, hi], axis=0)

    def step(i, carry):
        copy(i).wait()
        at = pl.ds(pl.multiple_of(i * CHUNK, CHUNK), CHUNK)
        hi, mid = split(xbuf[at, :])
        obuf[at, :] = fast(jnp.concatenate([hi, hi, mid], axis=1), proj[...]).astype(jnp.bfloat16)
        out(i).start()
        return carry

    lax.fori_loop(0, chunks, step, 0)
    for i in range(chunks):
        out(i).wait()


def local(n_grp, n_leaf, x, sketch):
    rows, cols = x.shape
    modes = sketch.shape[1]
    chunks = rows // CHUNK
    f32 = jnp.float32
    hbm = pl.BlockSpec(memory_space=pl.ANY)
    dma = pltpu.SemaphoreType.DMA
    piece = (modes * cols // (n_leaf * LANES), LANES)
    yt = pl.pallas_call(
        functools.partial(merge_kernel, n_grp, n_leaf),
        out_shape=jax.ShapeDtypeStruct((modes, cols), f32),
        in_specs=[hbm, VMEM],
        out_specs=VMEM,
        scratch_shapes=[
            pltpu.VMEM((rows, cols), f32), pltpu.VMEM((cols, 2 * cols), f32), pltpu.VMEM((cols, cols), f32),
            pltpu.VMEM((modes, 2 * modes), f32),
            pltpu.VMEM((n_grp, modes, cols), f32), pltpu.VMEM((n_grp, modes, modes), f32),
            pltpu.VMEM((n_leaf, *piece), f32), pltpu.VMEM((n_leaf - 1, *piece), f32),
            pltpu.VMEM(piece, f32), pltpu.VMEM((n_leaf, *piece), f32),
            dma((chunks,)), dma((2, n_grp - 1)), dma((2, n_grp - 1)), dma((2, n_leaf - 1)), dma((2, n_leaf - 1)),
        ],
        compiler_params=pltpu.CompilerParams(collective_id=0, has_side_effects=True),
    )(x, sketch.T)
    return pl.pallas_call(
        project_kernel,
        out_shape=jax.ShapeDtypeStruct((rows, cols), jnp.bfloat16),
        in_specs=[hbm, VMEM],
        out_specs=hbm,
        scratch_shapes=[
            pltpu.VMEM((rows, cols), f32), pltpu.VMEM((rows, cols), jnp.bfloat16),
            pltpu.VMEM((3 * cols, cols), jnp.bfloat16),
            pltpu.VMEM((modes, 2 * modes), f32), dma((chunks,)), dma((chunks,)),
        ],
    )(x, yt)


def solution(mesh):
    return jax.shard_map(
        functools.partial(local, mesh.shape["grp"], mesh.shape["leaf"]),
        mesh=mesh,
        in_specs=(P(("grp", "leaf"), None), P()),
        out_specs=P(("grp", "leaf"), None),
        check_vma=False,
    )
```
